128 devices in a mesh: dp: 16 (over z, y), ep: 8 (over x, core).
Axes of the slice: x: 4, y: 4, z: 4, core: 2. Of those that a mesh axis runs over, the one named last changes fastest.
Arguments:
- hidden: bfloat16 [8192, 2304], P(('dp', 'ep'))
- grad_out: bfloat16 [8192, 2304], P(('dp', 'ep'))
- expert_ids: int32 [8192, 2], P(('dp', 'ep'))
- norm_gain: float32 [2304], replicated
- w_router: float32 [2304, 8], replicated
- w_gate: bfloat16 [8, 2304, 5760], P('ep')
- w_up: bfloat16 [8, 2304, 5760], P('ep')
- w_down: bfloat16 [8, 5760, 2304], P('ep')
Outputs:
- output 1: bfloat16 [8192, 2304], P(('dp', 'ep'))
- output 2: float32 [], replicated
- output 3: bfloat16 [8192, 2304], P(('dp', 'ep'))
- output 4: float32 [2304], replicated
- output 5: float32 [2304, 8], replicated
- output 6: bfloat16 [8, 2304, 5760], P('ep')
- output 7: bfloat16 [8, 2304, 5760], P('ep')
- output 8: bfloat16 [8, 5760, 2304], P('ep')
All inputs are finite; a program needn't handle non-finite values.
Results may differ from the reference program's by a relative error of at most 0.0141986.
Values are sent between devices in bfloat16 or wider.
A program may use at most 1 GiB of HBM per device.

```python
import functools
import jax
import jax.numpy as jnp
from jax import lax

D = 2304
FF = 5760
EXPERTS = 8
TOK = 64
DEVICES = 128
CAP = 4 * TOK // EXPERTS
ROWS_EXP = DEVICES * CAP
S_ALL = TOK * DEVICES
EPS = 1e-6
AUX_COEF = 0.001


def draw_routes(key):
    key_order, key_shift, key_perm, key_swap = jax.random.split(key, 4)
    half_exp = EXPERTS // 2
    mean_load = 2 * TOK // EXPERTS
    shift = jax.random.randint(key_shift, (DEVICES, half_exp), 0, mean_load + 1)
    shift = shift.at[:, 0].set(mean_load)
    order = jax.vmap(lambda sub_key: jax.random.permutation(sub_key, EXPERTS))(jax.random.split(key_order, DEVICES))
    signed = jnp.concatenate([shift, -shift], axis=1)
    expert_range = jnp.arange(EXPERTS, dtype=jnp.int32)
    loads = mean_load + jnp.sum(signed[:, :, None] * (order[:, :, None] == expert_range).astype(jnp.int32), axis=1)
    bounds = jnp.cumsum(loads, axis=1)
    positions = jnp.arange(2 * TOK, dtype=jnp.int32)
    listed = jax.vmap(lambda bound_row: jnp.searchsorted(bound_row, positions, side="right"))(bounds).astype(jnp.int32)
    token_order = jax.vmap(lambda sub_key: jax.random.permutation(sub_key, TOK))(jax.random.split(key_perm, DEVICES))
    first = jnp.take_along_axis(listed[:, :TOK], token_order, axis=1)
    second = jnp.take_along_axis(listed[:, TOK:], token_order, axis=1)
    swap = jax.random.randint(key_swap, (DEVICES, TOK), 0, 2) == 1
    id_first = jnp.where(swap, second, first)
    id_second = jnp.where(swap, first, second)
    return jnp.stack([id_first, id_second], axis=-1).reshape(DEVICES * TOK, 2).astype(jnp.int32)


def setup_inputs(seed: int = 0) -> dict:
    key = jax.random.key(seed)
    keys = jax.random.split(key, 8)
    expert_ids = draw_routes(keys[0])
    w_router = jax.random.normal(keys[1], (D, EXPERTS), jnp.float32) * D ** -0.5
    col_dir = w_router * lax.rsqrt(jnp.mean(w_router * w_router, axis=0, keepdims=True))
    chosen = jnp.sum((expert_ids[:, :, None] == jnp.arange(EXPERTS, dtype=jnp.int32)).astype(jnp.float32), axis=1)
    boost = jnp.dot(chosen, col_dir.T, preferred_element_type=jnp.float32)
    hidden = jax.random.normal(keys[2], (S_ALL, D), jnp.float32) + (2.5 * D ** -0.5) * boost
    grad_out = jax.random.normal(keys[3], (S_ALL, D), jnp.float32)
    norm_gain = 1.0 + 0.3 * jax.random.normal(keys[4], (D,), jnp.float32)
    w_gate = jax.random.normal(keys[5], (EXPERTS, D, FF), jnp.float32) * D ** -0.5
    w_up = jax.random.normal(keys[6], (EXPERTS, D, FF), jnp.float32) * D ** -0.5
    w_down = jax.random.normal(keys[7], (EXPERTS, FF, D), jnp.float32) * (2.0 * FF ** -0.5)
    return {"hidden": hidden.astype(jnp.bfloat16), "grad_out": grad_out.astype(jnp.bfloat16), "expert_ids": expert_ids, "norm_gain": norm_gain, "w_router": w_router, "w_gate": w_gate.astype(jnp.bfloat16), "w_up": w_up.astype(jnp.bfloat16), "w_down": w_down.astype(jnp.bfloat16)}


def bf16_trip(value):
    return value.astype(jnp.bfloat16).astype(jnp.float32)


def route_tables(expert_ids, n_exp, capacity):
    flat_ids = expert_ids.reshape(-1)
    n_choice = flat_ids.shape[0]
    one_hot = (flat_ids[:, None] == jnp.arange(n_exp, dtype=jnp.int32)[None, :]).astype(jnp.int32)
    running = jnp.cumsum(one_hot, axis=0) - 1
    dest_rows = flat_ids * capacity + jnp.sum(running * one_hot, axis=1)
    slot_owner = jnp.full((n_exp * capacity,), n_choice, jnp.int32).at[dest_rows].set(jnp.arange(n_choice, dtype=jnp.int32))
    return dest_rows, slot_owner, jnp.sum(one_hot, axis=0)


def expert_ffn(operands):
    rows, gate_w, up_w, down_w = operands
    h_gate = bf16_trip(jnp.dot(rows, gate_w.astype(jnp.float32), preferred_element_type=jnp.float32))
    h_up = bf16_trip(jnp.dot(rows, up_w.astype(jnp.float32), preferred_element_type=jnp.float32))
    act_rows = bf16_trip(jax.nn.silu(h_gate) * h_up)
    return bf16_trip(jnp.dot(act_rows, down_w.astype(jnp.float32), preferred_element_type=jnp.float32))


def forward_pass(hidden, norm_gain, w_router, w_gate, w_up, w_down, expert_ids):
    dest_rows, slot_owner, loads = route_tables(expert_ids, EXPERTS, ROWS_EXP)
    choice_hot = (expert_ids[:, :, None] == jnp.arange(EXPERTS, dtype=jnp.int32)).astype(jnp.float32)
    x_f32 = hidden.astype(jnp.float32)
    inv_rms = lax.rsqrt(jnp.mean(x_f32 * x_f32, axis=-1, keepdims=True) + EPS)
    x_norm = bf16_trip(x_f32 * inv_rms * norm_gain)
    logits = jnp.dot(x_norm, w_router, preferred_element_type=jnp.float32)
    router_probs = jax.nn.softmax(logits, axis=-1)
    gate_vals = jnp.sum(router_probs[:, None, :] * choice_hot, axis=-1)
    rows = bf16_trip(jnp.take(x_norm, slot_owner // 2, axis=0, mode="fill", fill_value=0))
    exp_out = lax.map(jax.checkpoint(expert_ffn), (rows.reshape(EXPERTS, ROWS_EXP, D), w_gate, w_up, w_down))
    picked = jnp.take(exp_out.reshape(EXPERTS * ROWS_EXP, D), dest_rows, axis=0).reshape(S_ALL, 2, D)
    out_hidden = (x_f32 + jnp.sum(gate_vals[:, :, None] * picked, axis=1)).astype(jnp.bfloat16)
    load_frac = loads.astype(jnp.float32) / (2 * S_ALL)
    aux_loss = AUX_COEF * EXPERTS * jnp.sum(load_frac * jnp.mean(router_probs, axis=0))
    return out_hidden, aux_loss


def reference(hidden, grad_out, expert_ids, norm_gain, w_router, w_gate, w_up, w_down):
    forward_fn = functools.partial(forward_pass, expert_ids=expert_ids)
    (out_hidden, aux_loss), pullback = jax.vjp(forward_fn, hidden, norm_gain, w_router, w_gate, w_up, w_down)
    all_grads = pullback((grad_out, jnp.ones_like(aux_loss)))
    return (out_hidden, aux_loss, all_grads[0], all_grads[1], all_grads[2], all_grads[3], all_grads[4], all_grads[5])
```

```python
import functools
import jax
import jax.numpy as jnp
from jax import lax
from jax.experimental import pallas as pl
from jax.experimental.pallas import tpu as pltpu
from jax.sharding import PartitionSpec as P

EPS = 1e-6
AUX_COEF = 0.001
ROWS = 256
TILE = 384
SLICE = 192
NT = (((1,), (1,)), ((), ()))


def route_tables(expert_ids, n_exp, capacity):
    flat_ids = expert_ids.reshape(-1)
    n_choice = flat_ids.shape[0]
    one_hot = (flat_ids[:, None] == jnp.arange(n_exp, dtype=jnp.int32)[None, :]).astype(jnp.int32)
    running = jnp.cumsum(one_hot, axis=0) - 1
    dest_rows = flat_ids * capacity + jnp.sum(running * one_hot, axis=1)
    slot_owner = jnp.full((n_exp * capacity,), n_choice, jnp.int32).at[dest_rows].set(jnp.arange(n_choice, dtype=jnp.int32))
    return dest_rows, slot_owner


def pack_kernel(block_of, chunk_of, n_steps, tok_ref, pos_ref, gate_ref, x_ref, d_ref, acc, gacc):
    step = pl.program_id(0)
    width = x_ref.shape[1]
    block = block_of[step]

    @pl.when((step == 0) | (block != block_of[jnp.maximum(step - 1, 0)]))
    def _():
        acc[...] = jnp.zeros_like(acc)
        gacc[...] = jnp.zeros_like(gacc)

    @pl.when(step < n_steps[0])
    def _():
        rows = tok_ref.shape[0]
        row_id = block * rows + lax.broadcasted_iota(jnp.int32, (rows, rows), 0)
        hit = pos_ref[0] == row_id
        acc[...] += jnp.dot(hit.astype(jnp.float32).astype(jnp.bfloat16), tok_ref[...], preferred_element_type=jnp.float32)
        gacc[...] += jnp.sum(jnp.where(hit, gate_ref[0], 0.0), axis=1, keepdims=True)

    @pl.when((step == n_steps[0] - 1) | ((step < n_steps[0]) & (block != block_of[step + 1])))
    def _():
        x_ref[...] = acc[:, :width].astype(jnp.bfloat16)
        d_ref[...] = (acc[:, width:] * gacc[...]).astype(jnp.bfloat16)


def pack_rows(tokens, mask, gate, cap):
    n_tok, two_d = tokens.shape
    width = two_d // 2
    n_chunk = n_tok // ROWS
    n_block = cap // ROWS
    m = mask.astype(jnp.bfloat16).reshape(n_chunk, ROWS)
    idx = jnp.arange(ROWS)
    inside = jnp.dot(m, (idx[:, None] < idx[None, :]).astype(jnp.bfloat16), preferred_element_type=jnp.float32).astype(jnp.int32)
    per_chunk = jnp.sum(mask.astype(jnp.int32).reshape(n_chunk, ROWS), axis=1)
    cidx = jnp.arange(n_chunk)
    ends = jnp.sum(jnp.where(cidx[None, :] <= cidx[:, None], per_chunk[None, :], 0), axis=1)
    pos = jnp.where(mask.reshape(n_chunk, ROWS), inside + (ends - per_chunk)[:, None], -1)
    count = jnp.sum(per_chunk)
    n_used = jnp.maximum((count + ROWS - 1) // ROWS, 1)
    bidx = jnp.arange(n_block)
    last_row = jnp.minimum((bidx + 1) * ROWS, count) - 1
    last_chunk = jnp.sum((ends[None, :] <= last_row[:, None]).astype(jnp.int32), axis=1)
    n_steps = jnp.sum(jnp.where(bidx == n_used - 1, last_chunk + bidx, 0)) + 1
    steps = jnp.arange(n_chunk + n_block + 1)
    block_of = jnp.minimum(jnp.sum(((last_chunk + bidx)[None, :] < steps[:, None]).astype(jnp.int32), axis=1), n_used - 1)
    chunk_of = jnp.clip(steps - block_of, 0, n_chunk - 1)
    grid_spec = pltpu.PrefetchScalarGridSpec(
        num_scalar_prefetch=3,
        grid=(n_chunk + n_block,),
        in_specs=[
            pl.BlockSpec((ROWS, two_d), lambda s, b, c, n: (c[s], 0)),
            pl.BlockSpec((1, 1, ROWS), lambda s, b, c, n: (c[s], 0, 0)),
            pl.BlockSpec((1, 1, ROWS), lambda s, b, c, n: (c[s], 0, 0)),
        ],
        out_specs=[pl.BlockSpec((ROWS, width), lambda s, b, c, n: (b[s], 0))] * 2,
        scratch_shapes=[pltpu.VMEM((ROWS, two_d), jnp.float32), pltpu.VMEM((ROWS, 1), jnp.float32)],
    )
    x_rows, d_rows = pl.pallas_call(
        pack_kernel,
        grid_spec=grid_spec,
        out_shape=[jax.ShapeDtypeStruct((cap, width), jnp.bfloat16)] * 2,
        compiler_params=pltpu.CompilerParams(dimension_semantics=("arbitrary",), vmem_limit_bytes=40 * 2**20),
        cost_estimate=pl.CostEstimate(flops=2 * 5 * ROWS * cap * two_d // 2, bytes_accessed=2 * n_tok * two_d * 2, transcendentals=0),
        name="pack_rows",
    )(block_of.astype(jnp.int32), chunk_of.astype(jnp.int32), n_steps.astype(jnp.int32)[None], tokens, pos.astype(jnp.int32)[:, None, :], gate.reshape(n_chunk, 1, ROWS))
    return x_rows, d_rows, n_used.astype(jnp.int32)[None]


def weight_grad_step(wt, wd, x, d, acc_gu, acc_d):
    f = wd.shape[0]
    h = lax.dot_general(wt, x, NT, preferred_element_type=jnp.float32)
    hg = h[:f].astype(jnp.bfloat16).astype(jnp.float32)
    hu = h[f:].astype(jnp.bfloat16).astype(jnp.float32)
    da = lax.dot_general(wd, d, NT, preferred_element_type=jnp.float32).astype(jnp.bfloat16).astype(jnp.float32)
    sig = jax.nn.sigmoid(hg)
    silu = hg * sig
    act = (silu * hu).astype(jnp.bfloat16)
    dhu = (da * silu).astype(jnp.bfloat16)
    dhg = (da * hu * sig * (1.0 + hg * (1.0 - sig))).astype(jnp.bfloat16)
    acc_gu[...] += jnp.dot(jnp.concatenate([dhg, dhu], axis=0), x, preferred_element_type=jnp.float32)
    acc_d[...] += jnp.dot(act, d, preferred_element_type=jnp.float32)


def slice_kernel(n_used, x_ref, d_ref, wt_ref, wd_ref, out_ref, acc_gu, acc_d):
    b = pl.program_id(0)

    @pl.when(b == 0)
    def _():
        acc_gu[...] = jnp.zeros_like(acc_gu)
        acc_d[...] = jnp.zeros_like(acc_d)

    @pl.when(b < n_used[0])
    def _():
        weight_grad_step(wt_ref[...], wd_ref[...], x_ref[...], d_ref[...], acc_gu, acc_d)

    @pl.when(b == pl.num_programs(0) - 1)
    def _():
        f2 = acc_gu.shape[0]
        out_ref[:f2] = acc_gu[...].astype(jnp.bfloat16)
        out_ref[f2:] = acc_d[...].astype(jnp.bfloat16)


def slice_grads(x_rows, d_rows, n_used, wt, wd):
    cap, width = x_rows.shape
    f = wd.shape[0]
    return pl.pallas_call(
        slice_kernel,
        grid_spec=pltpu.PrefetchScalarGridSpec(
            num_scalar_prefetch=1,
            grid=(cap // ROWS,),
            in_specs=[
                pl.BlockSpec((ROWS, width), lambda b, n: (jnp.minimum(b, n[0] - 1), 0)),
                pl.BlockSpec((ROWS, width), lambda b, n: (jnp.minimum(b, n[0] - 1), 0)),
                pl.BlockSpec((2 * f, width), lambda b, n: (0, 0)),
                pl.BlockSpec((f, width), lambda b, n: (0, 0)),
            ],
            out_specs=pl.BlockSpec((3 * f, width), lambda b, n: (0, 0)),
            scratch_shapes=[pltpu.VMEM((2 * f, width), jnp.float32), pltpu.VMEM((f, width), jnp.float32)],
        ),
        out_shape=jax.ShapeDtypeStruct((3 * f, width), jnp.bfloat16),
        compiler_params=pltpu.CompilerParams(dimension_semantics=("arbitrary",), vmem_limit_bytes=50 * 2**20),
        cost_estimate=pl.CostEstimate(flops=12 * (cap // 2) * width * f, bytes_accessed=cap * width * 2, transcendentals=0),
        name="slice_grads",
    )(n_used, x_rows, d_rows, wt, wd)


def tile_kernel(n_used, x_ref, d_ref, wg_ref, wu_ref, wd_ref, gg_ref, gu_ref, gd_ref, wt, acc_gu, acc_d):
    b = pl.program_id(1)
    f = wd_ref.shape[0]

    @pl.when(b == 0)
    def _():
        wt[:f] = wg_ref[...].T
        wt[f:] = wu_ref[...].T
        acc_gu[...] = jnp.zeros_like(acc_gu)
        acc_d[...] = jnp.zeros_like(acc_d)

    @pl.when(b < n_used[0])
    def _():
        weight_grad_step(wt[...], wd_ref[...], x_ref[...], d_ref[...], acc_gu, acc_d)

    @pl.when(b == pl.num_programs(1) - 1)
    def _():
        gg_ref[...] = acc_gu[:f].astype(jnp.bfloat16).T
        gu_ref[...] = acc_gu[f:].astype(jnp.bfloat16).T
        gd_ref[...] = acc_d[...].astype(jnp.bfloat16)


def tile_grads(x_rows, d_rows, n_used, w_gate, w_up, w_down, n_tile):
    cap, width = x_rows.shape
    ff = w_gate.shape[1]
    row_spec = pl.BlockSpec((ROWS, width), lambda j, b, n: (jnp.minimum(b, n[0] - 1), 0))
    col_spec = pl.BlockSpec((width, TILE), lambda j, b, n: (0, j))
    down_spec = pl.BlockSpec((TILE, width), lambda j, b, n: (j, 0))
    return pl.pallas_call(
        tile_kernel,
        grid_spec=pltpu.PrefetchScalarGridSpec(
            num_scalar_prefetch=1,
            grid=(n_tile, cap // ROWS),
            in_specs=[row_spec, row_spec, col_spec, col_spec, down_spec],
            out_specs=[col_spec, col_spec, down_spec],
            scratch_shapes=[pltpu.VMEM((2 * TILE, width), jnp.bfloat16), pltpu.VMEM((2 * TILE, width), jnp.float32), pltpu.VMEM((TILE, width), jnp.float32)],
        ),
        out_shape=[jax.ShapeDtypeStruct((width, ff), jnp.bfloat16)] * 2 + [jax.ShapeDtypeStruct((ff, width), jnp.bfloat16)],
        compiler_params=pltpu.CompilerParams(dimension_semantics=("arbitrary", "arbitrary"), vmem_limit_bytes=60 * 2**20),
        cost_estimate=pl.CostEstimate(flops=12 * (cap // 2) * width * TILE * n_tile, bytes_accessed=n_tile * cap * width * 2, transcendentals=0),
        name="tile_grads",
    )(n_used, x_rows, d_rows, w_gate, w_up, w_down)


def place_kernel(part_ref, gg_in, gu_in, gd_in, gg_ref, gu_ref, gd_ref):
    f = SLICE
    gg_ref[...] = jnp.concatenate([part_ref[0, :f], part_ref[1, :f]], axis=0).T
    gu_ref[...] = jnp.concatenate([part_ref[0, f:2 * f], part_ref[1, f:2 * f]], axis=0).T
    gd_ref[:f] = part_ref[0, 2 * f:]
    gd_ref[f:] = part_ref[1, 2 * f:]


def place_slices(parts, g_gate, g_up, g_down, n_tile):
    n_part, _, width = parts.shape
    col_spec = pl.BlockSpec((width, 2 * SLICE), lambda i: (0, n_tile + i))
    down_spec = pl.BlockSpec((2 * SLICE, width), lambda i: (n_tile + i, 0))
    any_spec = pl.BlockSpec(memory_space=pl.ANY)
    return pl.pallas_call(
        place_kernel,
        grid=(n_part // 2,),
        in_specs=[pl.BlockSpec((2, 3 * SLICE, width), lambda i: (i, 0, 0)), any_spec, any_spec, any_spec],
        out_specs=[col_spec, col_spec, down_spec],
        out_shape=[jax.ShapeDtypeStruct(g.shape, g.dtype) for g in (g_gate, g_up, g_down)],
        input_output_aliases={1: 0, 2: 1, 3: 2},
        compiler_params=pltpu.CompilerParams(dimension_semantics=("arbitrary",), vmem_limit_bytes=50 * 2**20),
        cost_estimate=pl.CostEstimate(flops=10**6, bytes_accessed=4 * parts.size, transcendentals=0),
        name="place_slices",
    )(parts, g_gate, g_up, g_down)


def solution(mesh):
    n_dp, n_ep = mesh.shape["dp"], mesh.shape["ep"]
    n_dev = n_dp * n_ep
    all_axes = ("dp", "ep")

    def local_step(hidden, grad_out, expert_ids, norm_gain, w_router, w_gate, w_up, w_down):
        n_tok, width = hidden.shape
        n_exp = w_router.shape[1]
        capacity = 4 * n_tok // n_exp
        total_tok = n_tok * n_dev
        w_gate, w_up, w_down = w_gate[0], w_up[0], w_down[0]
        ff = w_gate.shape[1]
        n_tile = (ff - SLICE * n_dp) // TILE
        my_exp = lax.axis_index("ep")
        dest_rows, slot_owner = route_tables(expert_ids, n_exp, capacity)
        choice_hot = (expert_ids[:, :, None] == jnp.arange(n_exp, dtype=jnp.int32)).astype(jnp.float32)

        x_f32 = hidden.astype(jnp.float32)
        inv_rms = lax.rsqrt(jnp.mean(x_f32 * x_f32, axis=-1, keepdims=True) + EPS)
        x_hat = x_f32 * inv_rms
        x_norm = (x_hat * norm_gain).astype(jnp.bfloat16)
        xn_f32 = x_norm.astype(jnp.float32)

        tokens = lax.all_gather(jnp.concatenate([x_norm, grad_out], axis=1), all_axes, axis=0, tiled=True)

        router_probs = jax.nn.softmax(jnp.dot(xn_f32, w_router, preferred_element_type=jnp.float32), axis=-1)
        gate_vals = jnp.sum(router_probs[:, None, :] * choice_hot, axis=-1)
        pad = jnp.zeros((n_tok, 16 - n_exp - 2), jnp.float32)
        routes = lax.all_gather(jnp.concatenate([router_probs, expert_ids.astype(jnp.float32), pad], axis=1), all_axes, axis=0, tiled=True)
        all_probs, all_ids = routes[:, :n_exp], routes[:, n_exp:n_exp + 2].astype(jnp.int32)
        exp_range = jnp.arange(n_exp, dtype=jnp.int32)
        loads = jnp.sum((all_ids[:, 0:1] == exp_range).astype(jnp.float32) + (all_ids[:, 1:2] == exp_range).astype(jnp.float32), axis=0)
        load_frac = loads / (2 * total_tok)
        aux_loss = AUX_COEF * n_exp * jnp.sum(load_frac * jnp.sum(all_probs, axis=0) / total_tok)

        dy_f32 = grad_out.astype(jnp.float32)
        d_picked = (dy_f32[:, None, :] * gate_vals[:, :, None]).astype(jnp.bfloat16).reshape(n_tok * 2, width)
        send_x = jnp.take(x_norm, slot_owner // 2, axis=0, mode="fill", fill_value=0)
        send_d = jnp.take(d_picked, slot_owner, axis=0, mode="fill", fill_value=0)
        send = jnp.concatenate([send_x, send_d], axis=1).reshape(n_exp, capacity, 2 * width)
        recv = lax.all_to_all(send, "ep", 0, 0, tiled=True).reshape(n_exp * capacity, 2 * width)
        recv_rows, d_recv = recv[:, :width], recv[:, width:]
        h_gate = jnp.dot(recv_rows, w_gate, preferred_element_type=jnp.float32).astype(jnp.bfloat16)
        h_up = jnp.dot(recv_rows, w_up, preferred_element_type=jnp.float32).astype(jnp.bfloat16)
        gate_f32 = h_gate.astype(jnp.float32)
        up_f32 = h_up.astype(jnp.float32)
        sig_gate = jax.nn.sigmoid(gate_f32)
        silu_gate = gate_f32 * sig_gate
        act_rows = (silu_gate * up_f32).astype(jnp.bfloat16)
        exp_out = jnp.dot(act_rows, w_down, preferred_element_type=jnp.float32).astype(jnp.bfloat16)
        d_act = lax.dot_general(d_recv, w_down, NT, preferred_element_type=jnp.float32)
        d_act = d_act.astype(jnp.bfloat16).astype(jnp.float32)
        d_hup = (d_act * silu_gate).astype(jnp.bfloat16)
        d_hgate = (d_act * up_f32 * sig_gate * (1.0 + gate_f32 * (1.0 - sig_gate))).astype(jnp.bfloat16)
        d_rows = (lax.dot_general(d_hgate, w_gate, NT, preferred_element_type=jnp.float32) + lax.dot_general(d_hup, w_up, NT, preferred_element_type=jnp.float32)).astype(jnp.bfloat16)
        home = jnp.concatenate([exp_out, d_rows], axis=1).reshape(n_exp, capacity, 2 * width)
        back = lax.all_to_all(home, "ep", 0, 0, tiled=True).reshape(n_exp * capacity, 2 * width)
        taken = jnp.take(back, dest_rows, axis=0).reshape(n_tok, 2, 2 * width)
        picked, d_xn_exp = taken[:, :, :width], taken[:, :, width:]
        out_hidden = (x_f32 + jnp.sum(gate_vals[:, :, None] * picked, axis=1)).astype(jnp.bfloat16)

        d_gates = jnp.sum(dy_f32[:, None, :] * picked, axis=-1)
        d_probs = jnp.sum(d_gates[:, :, None] * choice_hot, axis=1) + (AUX_COEF * n_exp / total_tok) * load_frac
        d_logits = router_probs * (d_probs - jnp.sum(router_probs * d_probs, axis=-1, keepdims=True))
        d_xnorm = jnp.einsum("te,de->td", d_logits, w_router) + d_xn_exp[:, 0].astype(jnp.float32) + d_xn_exp[:, 1].astype(jnp.float32)
        d_xnorm = d_xnorm.astype(jnp.bfloat16).astype(jnp.float32)
        scaled = d_xnorm * norm_gain
        grad_hidden = (inv_rms * (scaled - x_hat * jnp.mean(scaled * x_hat, axis=-1, keepdims=True)) + dy_f32).astype(jnp.bfloat16)
        small = jnp.concatenate([jnp.sum(d_xnorm * x_hat, axis=0)[None], jnp.einsum("te,td->ed", d_logits, xn_f32)], axis=0)
        small = lax.all_gather(small.reshape(-1, 128), all_axes, axis=0, tiled=True)
        small = jnp.sum(small.reshape(n_dev, -1, 128), axis=0).reshape(1 + n_exp, width)

        names = all_ids == my_exp
        mask = names[:, 0] | names[:, 1]
        gate = jnp.sum(jnp.where(exp_range == my_exp, all_probs, 0.0), axis=1)
        x_rows, do_rows, n_used = pack_rows(tokens, mask, gate, n_dev * capacity)
        at = n_tile * TILE + SLICE * lax.axis_index("dp")
        wt = jnp.concatenate([lax.dynamic_slice(w, (0, at), (width, SLICE)).T for w in (w_gate, w_up)], axis=0)
        mine = slice_grads(x_rows, do_rows, n_used, wt, lax.dynamic_slice(w_down, (at, 0), (SLICE, width)))
        parts = lax.all_gather(mine, "dp", axis=0, tiled=False)
        g_gate, g_up, g_down = tile_grads(x_rows, do_rows, n_used, w_gate, w_up, w_down, n_tile)
        g_gate, g_up, g_down = place_slices(parts, g_gate, g_up, g_down, n_tile)
        return (out_hidden, aux_loss, grad_hidden, small[0], small[1:].T, g_gate[None], g_up[None], g_down[None])

    tok_spec = P(all_axes, None)
    w_spec = P("ep", None, None)
    return jax.shard_map(local_step, mesh=mesh, in_specs=(tok_spec, tok_spec, tok_spec, P(), P(), w_spec, w_spec, w_spec), out_specs=(tok_spec, P(), tok_spec, P(), P(), w_spec, w_spec, w_spec), check_vma=False)
```

```python
import functools
import jax
import jax.numpy as jnp
from jax import lax
from jax.experimental import pallas as pl
from jax.experimental.pallas import tpu as pltpu
from jax.sharding import PartitionSpec as P

EPS = 1e-6
AUX_COEF = 0.001
ROWS = 256
GROUP = 2
CHUNK = 512
STRIP = 512
BUFFERS = 3
OWN_TILE = 640
TILE = 384
SLICE = 192
NT = (((1,), (1,)), ((), ()))


def route_tables(expert_ids, n_exp, capacity):
    flat_ids = expert_ids.reshape(-1)
    n_choice = flat_ids.shape[0]
    one_hot = (flat_ids[:, None] == jnp.arange(n_exp, dtype=jnp.int32)[None, :]).astype(jnp.int32)
    running = jnp.cumsum(one_hot, axis=0) - 1
    dest_rows = flat_ids * capacity + jnp.sum(running * one_hot, axis=1)
    slot_owner = jnp.full((n_exp * capacity,), n_choice, jnp.int32).at[dest_rows].set(jnp.arange(n_choice, dtype=jnp.int32))
    return dest_rows, slot_owner


def pack_kernel(block_of, chunk_of, n_steps, my_exp, tok_hbm, pos_ref, wr_ref, x_ref, d_ref, acc, ring, sems):
    step = pl.program_id(0)
    rows, width = x_ref.shape
    block = block_of[step]
    active = step < n_steps[0]
    chunk = chunk_of[step]
    last_chunk = chunk_of[n_steps[0] - 1]

    def load(c):
        slot = lax.rem(c, BUFFERS)
        return pltpu.make_async_copy(tok_hbm.at[pl.ds(pl.multiple_of(c * CHUNK, CHUNK), CHUNK)], ring.at[slot], sems.at[slot])

    @pl.when(step == 0)
    def _():
        for c in range(BUFFERS - 1):
            pl.when(c <= last_chunk)(load(c).start)

    @pl.when(active & ((step == 0) | (chunk != chunk_of[jnp.maximum(step - 1, 0)])))
    def _():
        load(chunk).wait()
        pl.when(chunk + BUFFERS - 1 <= last_chunk)(load(chunk + BUFFERS - 1).start)

    tok_ref = ring.at[lax.rem(chunk, BUFFERS)]
    new = (step == 0) | (block != block_of[jnp.maximum(step - 1, 0)])

    @pl.when(active)
    def _():
        row_id = block * rows + lax.broadcasted_iota(jnp.int32, (rows, tok_ref.shape[0]), 0)
        hit = (pos_ref[0] == row_id).astype(jnp.float32).astype(jnp.bfloat16)
        for at in range(0, 2 * width, STRIP):
            cols = slice(at, at + STRIP)
            acc[:, cols] = jnp.where(new, 0.0, acc[:, cols]) + jnp.dot(hit, tok_ref[:, cols], preferred_element_type=jnp.float32)

    @pl.when((step == n_steps[0] - 1) | (active & (block != block_of[step + 1])))
    def _():
        x = acc[:, :width].astype(jnp.bfloat16)
        logits = jnp.dot(x, wr_ref[...], preferred_element_type=jnp.float32)
        lane = lax.broadcasted_iota(jnp.int32, logits.shape, 1)
        logits = jnp.where(lane < my_exp[1], logits, -jnp.inf)
        p = jnp.exp(logits - jnp.max(logits, axis=1, keepdims=True))
        gate = jnp.sum(jnp.where(lane == my_exp[0], p, 0.0), axis=1, keepdims=True) / jnp.sum(p, axis=1, keepdims=True)
        x_ref[...] = x
        d_ref[...] = (acc[:, width:] * gate).astype(jnp.bfloat16)


def pack_rows(tokens, width, mask, w_router, my_exp, cap):
    n_tok = tokens.shape[0]
    n_exp = w_router.shape[1]
    n_chunk = n_tok // CHUNK
    n_block = cap // ROWS
    m = mask.astype(jnp.bfloat16).reshape(n_chunk, CHUNK)
    idx = jnp.arange(CHUNK)
    inside = jnp.dot(m, (idx[:, None] < idx[None, :]).astype(jnp.bfloat16), preferred_element_type=jnp.float32).astype(jnp.int32)
    per_chunk = jnp.sum(mask.astype(jnp.int32).reshape(n_chunk, CHUNK), axis=1)
    cidx = jnp.arange(n_chunk)
    ends = jnp.sum(jnp.where(cidx[None, :] <= cidx[:, None], per_chunk[None, :], 0), axis=1)
    pos = jnp.where(mask.reshape(n_chunk, CHUNK), inside + (ends - per_chunk)[:, None], -1)
    count = jnp.sum(per_chunk)
    n_used = jnp.maximum((count + ROWS - 1) // ROWS, 1)
    bidx = jnp.arange(n_block)
    last_row = jnp.minimum((bidx + 1) * ROWS, count) - 1
    last_chunk = jnp.sum((ends[None, :] <= last_row[:, None]).astype(jnp.int32), axis=1)
    n_steps = jnp.sum(jnp.where(bidx == n_used - 1, last_chunk + bidx, 0)) + 1
    steps = jnp.arange(n_chunk + n_block + 1)
    block_of = jnp.minimum(jnp.sum(((last_chunk + bidx)[None, :] < steps[:, None]).astype(jnp.int32), axis=1), n_used - 1)
    chunk_of = jnp.clip(steps - block_of, 0, n_chunk - 1)
    chunk_of = jnp.where(steps < n_steps, chunk_of, n_chunk - 1)
    grid_spec = pltpu.PrefetchScalarGridSpec(
        num_scalar_prefetch=4,
        grid=(n_chunk + n_block,),
        in_specs=[
            pl.BlockSpec(memory_space=pl.ANY),
            pl.BlockSpec((1, 1, CHUNK), lambda s, b, c, n, e: (c[s], 0, 0)),
            pl.BlockSpec((width, 128), lambda s, b, c, n, e: (0, 0)),
        ],
        out_specs=[pl.BlockSpec((ROWS, width), lambda s, b, c, n, e: (b[s], 0))] * 2,
        scratch_shapes=[
            pltpu.VMEM((ROWS, 2 * width), jnp.float32),
            pltpu.VMEM((BUFFERS, CHUNK, 2 * width), jnp.bfloat16),
            pltpu.SemaphoreType.DMA((BUFFERS,)),
        ],
    )
    x_rows, d_rows = pl.pallas_call(
        pack_kernel,
        grid_spec=grid_spec,
        out_shape=[jax.ShapeDtypeStruct((cap, width), jnp.bfloat16)] * 2,
        compiler_params=pltpu.CompilerParams(dimension_semantics=("arbitrary",), vmem_limit_bytes=56 * 2**20),
        cost_estimate=pl.CostEstimate(flops=5 * CHUNK * cap * width, bytes_accessed=n_tok * width * 5, transcendentals=0),
        name="pack_rows",
    )(
        block_of.astype(jnp.int32),
        chunk_of.astype(jnp.int32),
        n_steps.astype(jnp.int32)[None],
        jnp.stack([my_exp, jnp.int32(n_exp)]),
        tokens,
        pos.astype(jnp.int32)[:, None, :],
        jnp.pad(w_router, ((0, 0), (0, 128 - n_exp))).astype(jnp.bfloat16),
    )
    return x_rows, d_rows, n_used.astype(jnp.int32)


def ffn_grads(hg, hu, da):
    hg, hu, da = (v.astype(jnp.bfloat16).astype(jnp.float32) for v in (hg, hu, da))
    sig = jax.nn.sigmoid(hg)
    silu = hg * sig
    act = (silu * hu).astype(jnp.bfloat16)
    dhu = (da * silu).astype(jnp.bfloat16)
    dhg = (da * hu * sig * (1.0 + hg * (1.0 - sig))).astype(jnp.bfloat16)
    return act, dhg, dhu


def own_kernel(r_ref, wg_ref, wu_ref, wd_ref, out_ref, wt_ref, acc_o, acc_x):
    j = pl.program_id(0)
    width = wd_ref.shape[1]
    x, d = r_ref[:, :width], r_ref[:, width:]

    @pl.when(j == 0)
    def _():
        acc_o[...] = jnp.zeros_like(acc_o)
        acc_x[...] = jnp.zeros_like(acc_x)

    wt_ref[0] = wg_ref[...].T
    wt_ref[1] = wu_ref[...].T
    hg = jnp.dot(x, wg_ref[...], preferred_element_type=jnp.float32)
    hu = jnp.dot(x, wu_ref[...], preferred_element_type=jnp.float32)
    da = lax.dot_general(wd_ref[...], d, NT, preferred_element_type=jnp.float32).astype(jnp.bfloat16).T
    act, dhg, dhu = ffn_grads(hg, hu, da)
    acc_o[...] += jnp.dot(act, wd_ref[...], preferred_element_type=jnp.float32)
    acc_x[...] += lax.dot_general(wg_ref[...], dhg, NT, preferred_element_type=jnp.float32) + lax.dot_general(wu_ref[...], dhu, NT, preferred_element_type=jnp.float32)

    @pl.when(j == pl.num_programs(0) - 1)
    def _():
        out_ref[:, :width] = acc_o[...].astype(jnp.bfloat16)
        out_ref[:, width:] = acc_x[...].astype(jnp.bfloat16).T


def own_rows(recv, w_gate, w_up, w_down):
    rows, two_d = recv.shape
    width, ff = w_gate.shape
    f = OWN_TILE
    whole = pl.BlockSpec((rows, two_d), lambda j: (0, 0))
    col_spec = pl.BlockSpec((width, f), lambda j: (0, j))
    return pl.pallas_call(
        own_kernel,
        grid=(ff // f,),
        in_specs=[whole, col_spec, col_spec, pl.BlockSpec((f, width), lambda j: (j, 0))],
        out_specs=[whole, pl.BlockSpec((2, f, width), lambda j: (0, j, 0))],
        out_shape=[jax.ShapeDtypeStruct((rows, two_d), jnp.bfloat16), jax.ShapeDtypeStruct((2, ff, width), jnp.bfloat16)],
        scratch_shapes=[pltpu.VMEM((rows, width), jnp.float32), pltpu.VMEM((width, rows), jnp.float32)],
        compiler_params=pltpu.CompilerParams(dimension_semantics=("arbitrary",), vmem_limit_bytes=62 * 2**20),
        cost_estimate=pl.CostEstimate(flops=12 * rows * width * ff, bytes_accessed=6 * width * ff, transcendentals=0),
        name="own_rows",
    )(recv, w_gate, w_up, w_down)


def add_rows(wt, wd, x_ref, d_ref, acc_gu, acc_d, first, parts):
    f = wd.shape[0]
    acts, dgus = [], []
    for i in range(parts):
        x, d = x_ref[i * ROWS:(i + 1) * ROWS], d_ref[i * ROWS:(i + 1) * ROWS]
        h = lax.dot_general(wt, x, NT, preferred_element_type=jnp.float32)
        da = lax.dot_general(wd, d, NT, preferred_element_type=jnp.float32)
        act, dhg, dhu = ffn_grads(h[:f], h[f:], da)
        acts.append(act)
        dgus.append(jnp.concatenate([dhg, dhu], axis=0))
    act, dgu = (v[0] if parts == 1 else jnp.concatenate(v, axis=1) for v in (acts, dgus))
    x, d = x_ref[:parts * ROWS], d_ref[:parts * ROWS]
    acc_gu[...] = jnp.where(first, 0.0, acc_gu[...]) + jnp.dot(dgu, x, preferred_element_type=jnp.float32)
    acc_d[...] = jnp.where(first, 0.0, acc_d[...]) + jnp.dot(act, d, preferred_element_type=jnp.float32)


def tile_kernel(transpose, n_used, tile_of, block_of, x_ref, d_ref, wt_ref, wd_ref, *rest):
    outs, (acc_gu, acc_d) = rest[:-2], rest[-2:]
    f = wd_ref.shape[0]
    step = pl.program_id(0)
    block = block_of[step]
    active = step < n_used[1]
    left = n_used[0] - GROUP * block
    wt = wt_ref[...].reshape(2 * f, wd_ref.shape[1])
    for parts in range(1, GROUP + 1):
        fits = left >= parts if parts == GROUP else left == parts
        pl.when(active & fits)(functools.partial(add_rows, wt, wd_ref[...], x_ref, d_ref, acc_gu, acc_d, block == 0, parts))

    @pl.when(active & (left <= GROUP))
    def _():
        if transpose:
            outs[0][...] = acc_gu[:f].astype(jnp.bfloat16).T
            outs[1][...] = acc_gu[f:].astype(jnp.bfloat16).T
            outs[2][...] = acc_d[...].astype(jnp.bfloat16)
        else:
            outs[0][:2 * f] = acc_gu[...].astype(jnp.bfloat16)
            outs[0][2 * f:] = acc_d[...].astype(jnp.bfloat16)


def tile_grads(x_rows, d_rows, n_used, wt, wd, f, n_tile, ff):
    cap, width = x_rows.shape
    n_block = cap // (GROUP * ROWS)
    n_group = (n_used + GROUP - 1) // GROUP
    steps = jnp.arange(n_tile * n_block, dtype=jnp.int32)
    tile_of = jnp.minimum(steps // n_group, n_tile - 1)
    block_of = jnp.where(steps < n_tile * n_group, steps % n_group, n_group - 1)
    used = jnp.stack([n_used, n_tile * n_group])
    row_spec = pl.BlockSpec((GROUP * ROWS, width), lambda s, n, t, b: (b[s], 0))
    col_spec = pl.BlockSpec((width, f), lambda s, n, t, b: (0, t[s]))
    down_spec = pl.BlockSpec((f, width), lambda s, n, t, b: (t[s], 0))
    if ff:
        out_specs = [col_spec, col_spec, down_spec]
        out_shape = [jax.ShapeDtypeStruct((width, ff), jnp.bfloat16)] * 2 + [jax.ShapeDtypeStruct((ff, width), jnp.bfloat16)]
    else:
        out_specs = [pl.BlockSpec((3 * f, width), lambda s, n, t, b: (0, 0))]
        out_shape = [jax.ShapeDtypeStruct((3 * f, width), jnp.bfloat16)]
    return pl.pallas_call(
        functools.partial(tile_kernel, bool(ff)),
        grid_spec=pltpu.PrefetchScalarGridSpec(
            num_scalar_prefetch=3,
            grid=(n_tile * n_block,),
            in_specs=[row_spec, row_spec, pl.BlockSpec((2, f, width), lambda s, n, t, b: (0, t[s], 0)), down_spec],
            out_specs=out_specs,
            scratch_shapes=[pltpu.VMEM((2 * f, width), jnp.float32), pltpu.VMEM((f, width), jnp.float32)],
        ),
        out_shape=out_shape,
        compiler_params=pltpu.CompilerParams(dimension_semantics=("arbitrary",), vmem_limit_bytes=63 * 2**20),
        cost_estimate=pl.CostEstimate(flops=12 * (cap // 2) * width * f * n_tile, bytes_accessed=n_tile * cap * width * 2, transcendentals=0),
        name="tile_grads" if ff else "slice_grads",
    )(used, tile_of, block_of, x_rows, d_rows, wt, wd)


def place_kernel(part_ref, gg_in, gu_in, gd_in, gg_ref, gu_ref, gd_ref):
    f = SLICE
    gg_ref[...] = jnp.concatenate([part_ref[0, :f], part_ref[1, :f]], axis=0).T
    gu_ref[...] = jnp.concatenate([part_ref[0, f:2 * f], part_ref[1, f:2 * f]], axis=0).T
    gd_ref[:f] = part_ref[0, 2 * f:]
    gd_ref[f:] = part_ref[1, 2 * f:]


def place_slices(parts, g_gate, g_up, g_down, n_tile):
    n_part, _, width = parts.shape
    col_spec = pl.BlockSpec((width, 2 * SLICE), lambda i: (0, n_tile + i))
    down_spec = pl.BlockSpec((2 * SLICE, width), lambda i: (n_tile + i, 0))
    any_spec = pl.BlockSpec(memory_space=pl.ANY)
    return pl.pallas_call(
        place_kernel,
        grid=(n_part // 2,),
        in_specs=[pl.BlockSpec((2, 3 * SLICE, width), lambda i: (i, 0, 0)), any_spec, any_spec, any_spec],
        out_specs=[col_spec, col_spec, down_spec],
        out_shape=[jax.ShapeDtypeStruct(g.shape, g.dtype) for g in (g_gate, g_up, g_down)],
        input_output_aliases={1: 0, 2: 1, 3: 2},
        compiler_params=pltpu.CompilerParams(dimension_semantics=("arbitrary",), vmem_limit_bytes=50 * 2**20),
        cost_estimate=pl.CostEstimate(flops=10**6, bytes_accessed=4 * parts.size, transcendentals=0),
        name="place_slices",
    )(parts, g_gate, g_up, g_down)


def solution(mesh):
    n_dp, n_ep = mesh.shape["dp"], mesh.shape["ep"]
    n_dev = n_dp * n_ep
    all_axes = ("dp", "ep")

    def local_step(hidden, grad_out, expert_ids, norm_gain, w_router, w_gate, w_up, w_down):
        n_tok, width = hidden.shape
        n_exp = w_router.shape[1]
        capacity = 4 * n_tok // n_exp
        total_tok = n_tok * n_dev
        w_gate, w_up, w_down = w_gate[0], w_up[0], w_down[0]
        ff = w_gate.shape[1]
        n_tile = (ff - SLICE * n_dp) // TILE
        my_exp = lax.axis_index("ep")
        dest_rows, slot_owner = route_tables(expert_ids, n_exp, capacity)
        choice_hot = (expert_ids[:, :, None] == jnp.arange(n_exp, dtype=jnp.int32)).astype(jnp.float32)

        x_f32 = hidden.astype(jnp.float32)
        inv_rms = lax.rsqrt(jnp.mean(x_f32 * x_f32, axis=-1, keepdims=True) + EPS)
        x_hat = x_f32 * inv_rms
        x_norm = (x_hat * norm_gain).astype(jnp.bfloat16)
        xn_f32 = x_norm.astype(jnp.float32)

        tokens = lax.all_gather(jnp.concatenate([x_norm, grad_out], axis=1), all_axes, axis=0, tiled=True)

        router_probs = jax.nn.softmax(jnp.dot(xn_f32, w_router, preferred_element_type=jnp.float32), axis=-1)
        gate_vals = jnp.sum(router_probs[:, None, :] * choice_hot, axis=-1)
        pad = jnp.zeros((n_tok, 16 - n_exp - 2), jnp.float32)
        routes = lax.all_gather(jnp.concatenate([router_probs, expert_ids.astype(jnp.float32), pad], axis=1), all_axes, axis=0, tiled=True)
        all_probs, all_ids = routes[:, :n_exp], routes[:, n_exp:n_exp + 2].astype(jnp.int32)
        exp_range = jnp.arange(n_exp, dtype=jnp.int32)
        loads = jnp.sum((all_ids[:, 0:1] == exp_range).astype(jnp.float32) + (all_ids[:, 1:2] == exp_range).astype(jnp.float32), axis=0)
        load_frac = loads / (2 * total_tok)
        aux_loss = AUX_COEF * n_exp * jnp.sum(load_frac * jnp.sum(all_probs, axis=0) / total_tok)

        dy_f32 = grad_out.astype(jnp.float32)
        d_picked = (dy_f32[:, None, :] * gate_vals[:, :, None]).astype(jnp.bfloat16).reshape(n_tok * 2, width)
        send_x = jnp.take(x_norm, slot_owner // 2, axis=0, mode="fill", fill_value=0)
        send_d = jnp.take(d_picked, slot_owner, axis=0, mode="fill", fill_value=0)
        send = jnp.concatenate([send_x, send_d], axis=1).reshape(n_exp, capacity, 2 * width)
        recv = lax.all_to_all(send, "ep", 0, 0, tiled=True).reshape(n_exp * capacity, 2 * width)
        home, wt = own_rows(recv, w_gate, w_up, w_down)
        home = home.reshape(n_exp, capacity, 2 * width)
        back = lax.all_to_all(home, "ep", 0, 0, tiled=True).reshape(n_exp * capacity, 2 * width)
        taken = jnp.take(back, dest_rows, axis=0).reshape(n_tok, 2, 2 * width)
        picked, d_xn_exp = taken[:, :, :width], taken[:, :, width:]
        out_hidden = (x_f32 + jnp.sum(gate_vals[:, :, None] * picked, axis=1)).astype(jnp.bfloat16)

        d_gates = jnp.sum(dy_f32[:, None, :] * picked, axis=-1)
        d_probs = jnp.sum(d_gates[:, :, None] * choice_hot, axis=1) + (AUX_COEF * n_exp / total_tok) * load_frac
        d_logits = router_probs * (d_probs - jnp.sum(router_probs * d_probs, axis=-1, keepdims=True))
        d_xnorm = jnp.einsum("te,de->td", d_logits, w_router) + d_xn_exp[:, 0].astype(jnp.float32) + d_xn_exp[:, 1].astype(jnp.float32)
        d_xnorm = d_xnorm.astype(jnp.bfloat16).astype(jnp.float32)
        scaled = d_xnorm * norm_gain
        grad_hidden = (inv_rms * (scaled - x_hat * jnp.mean(scaled * x_hat, axis=-1, keepdims=True)) + dy_f32).astype(jnp.bfloat16)
        small = [jnp.sum(d_xnorm * x_hat, axis=0), jnp.einsum("te,td->ed", d_logits, xn_f32).reshape(-1)]
        small = lax.all_gather(jnp.concatenate(small).reshape(-1, 128), all_axes, axis=0, tiled=True)
        small = jnp.sum(small.reshape(n_dev, -1, 128), axis=0).reshape(1 + n_exp, width)

        at = n_tile * TILE + SLICE * lax.axis_index("dp")
        wt_mine = lax.dynamic_slice(wt, (0, at, 0), (2, SLICE, width))
        wd_mine = lax.dynamic_slice(w_down, (at, 0), (SLICE, width))
        names = all_ids == my_exp
        x_rows, do_rows, n_used = pack_rows(tokens, width, names[:, 0] | names[:, 1], w_router, my_exp, n_dev * capacity)
        (mine,) = tile_grads(x_rows, do_rows, n_used, wt_mine, wd_mine, SLICE, 1, 0)
        parts = lax.all_gather(mine, "dp", axis=0, tiled=False)
        grads = tile_grads(x_rows, do_rows, n_used, wt, w_down, TILE, n_tile, ff)
        g_gate, g_up, g_down = place_slices(parts, *grads, n_tile)
        return (out_hidden, aux_loss, grad_hidden, small[0], small[1:].T, g_gate[None], g_up[None], g_down[None])

    tok_spec = P(all_axes, None)
    w_spec = P("ep", None, None)
    return jax.shard_map(local_step, mesh=mesh, in_specs=(tok_spec, tok_spec, tok_spec, P(), P(), w_spec, w_spec, w_spec), out_specs=(tok_spec, P(), tok_spec, P(), P(), w_spec, w_spec, w_spec), check_vma=False)
```

```python
import functools
import jax
import jax.numpy as jnp
from jax import lax
from jax.experimental import pallas as pl
from jax.experimental.pallas import tpu as pltpu
from jax.sharding import PartitionSpec as P

EPS = 1e-6
AUX_COEF = 0.001
ROWS = 256
GROUP = 2
CHUNK = 512
STRIP = 512
BUFFERS = 3
OWN_TILE = 640
TILE = 384
SLICE = 192
NT = (((1,), (1,)), ((), ()))


def route_tables(expert_ids, n_exp, capacity):
    flat_ids = expert_ids.reshape(-1)
    n_choice = flat_ids.shape[0]
    one_hot = (flat_ids[:, None] == jnp.arange(n_exp, dtype=jnp.int32)[None, :]).astype(jnp.int32)
    running = jnp.cumsum(one_hot, axis=0) - 1
    dest_rows = flat_ids * capacity + jnp.sum(running * one_hot, axis=1)
    slot_owner = jnp.full((n_exp * capacity,), n_choice, jnp.int32).at[dest_rows].set(jnp.arange(n_choice, dtype=jnp.int32))
    return dest_rows, slot_owner


def pack_kernel(block_of, chunk_of, n_steps, my_exp, tok_hbm, pos_ref, wr_ref, x_ref, d_ref, acc, ring, sems):
    step = pl.program_id(0)
    rows, width = x_ref.shape
    block = block_of[step]
    active = step < n_steps[0]
    chunk = chunk_of[step]
    last_chunk = chunk_of[n_steps[0] - 1]

    def load(c):
        slot = lax.rem(c, BUFFERS)
        return pltpu.make_async_copy(tok_hbm.at[pl.ds(pl.multiple_of(c * CHUNK, CHUNK), CHUNK)], ring.at[slot], sems.at[slot])

    @pl.when(step == 0)
    def _():
        for c in range(BUFFERS - 1):
            pl.when(c <= last_chunk)(load(c).start)

    @pl.when(active & ((step == 0) | (chunk != chunk_of[jnp.maximum(step - 1, 0)])))
    def _():
        load(chunk).wait()
        pl.when(chunk + BUFFERS - 1 <= last_chunk)(load(chunk + BUFFERS - 1).start)

    tok_ref = ring.at[lax.rem(chunk, BUFFERS)]
    new = (step == 0) | (block != block_of[jnp.maximum(step - 1, 0)])

    @pl.when(active)
    def _():
        row_id = block * rows + lax.broadcasted_iota(jnp.int32, (rows, tok_ref.shape[0]), 0)
        hit = (pos_ref[0] == row_id).astype(jnp.float32).astype(jnp.bfloat16)
        for at in range(0, 2 * width, STRIP):
            cols = slice(at, at + STRIP)
            acc[:, cols] = jnp.where(new, 0.0, acc[:, cols]) + jnp.dot(hit, tok_ref[:, cols], preferred_element_type=jnp.float32)

    @pl.when((step == n_steps[0] - 1) | (active & (block != block_of[step + 1])))
    def _():
        x = acc[:, :width].astype(jnp.bfloat16)
        logits = jnp.dot(x, wr_ref[...], preferred_element_type=jnp.float32)
        lane = lax.broadcasted_iota(jnp.int32, logits.shape, 1)
        logits = jnp.where(lane < my_exp[1], logits, -jnp.inf)
        p = jnp.exp(logits - jnp.max(logits, axis=1, keepdims=True))
        gate = jnp.sum(jnp.where(lane == my_exp[0], p, 0.0), axis=1, keepdims=True) / jnp.sum(p, axis=1, keepdims=True)
        x_ref[...] = x
        d_ref[...] = (acc[:, width:] * gate).astype(jnp.bfloat16)


def pack_rows(tokens, width, mask, w_router, my_exp, cap):
    n_tok = tokens.shape[0]
    n_exp = w_router.shape[1]
    n_chunk = n_tok // CHUNK
    n_block = cap // ROWS
    m = mask.astype(jnp.bfloat16).reshape(n_chunk, CHUNK)
    idx = jnp.arange(CHUNK)
    inside = jnp.dot(m, (idx[:, None] < idx[None, :]).astype(jnp.bfloat16), preferred_element_type=jnp.float32).astype(jnp.int32)
    per_chunk = jnp.sum(mask.astype(jnp.int32).reshape(n_chunk, CHUNK), axis=1)
    cidx = jnp.arange(n_chunk)
    ends = jnp.sum(jnp.where(cidx[None, :] <= cidx[:, None], per_chunk[None, :], 0), axis=1)
    pos = jnp.where(mask.reshape(n_chunk, CHUNK), inside + (ends - per_chunk)[:, None], -1)
    count = jnp.sum(per_chunk)
    n_used = jnp.maximum((count + ROWS - 1) // ROWS, 1)
    bidx = jnp.arange(n_block)
    last_row = jnp.minimum((bidx + 1) * ROWS, count) - 1
    last_chunk = jnp.sum((ends[None, :] <= last_row[:, None]).astype(jnp.int32), axis=1)
    n_steps = jnp.sum(jnp.where(bidx == n_used - 1, last_chunk + bidx, 0)) + 1
    steps = jnp.arange(n_chunk + n_block + 1)
    block_of = jnp.minimum(jnp.sum(((last_chunk + bidx)[None, :] < steps[:, None]).astype(jnp.int32), axis=1), n_used - 1)
    chunk_of = jnp.clip(steps - block_of, 0, n_chunk - 1)
    chunk_of = jnp.where(steps < n_steps, chunk_of, n_chunk - 1)
    grid_spec = pltpu.PrefetchScalarGridSpec(
        num_scalar_prefetch=4,
        grid=(n_chunk + n_block,),
        in_specs=[
            pl.BlockSpec(memory_space=pl.ANY),
            pl.BlockSpec((1, 1, CHUNK), lambda s, b, c, n, e: (c[s], 0, 0)),
            pl.BlockSpec((width, 128), lambda s, b, c, n, e: (0, 0)),
        ],
        out_specs=[pl.BlockSpec((ROWS, width), lambda s, b, c, n, e: (b[s], 0))] * 2,
        scratch_shapes=[
            pltpu.VMEM((ROWS, 2 * width), jnp.float32),
            pltpu.VMEM((BUFFERS, CHUNK, 2 * width), jnp.bfloat16),
            pltpu.SemaphoreType.DMA((BUFFERS,)),
        ],
    )
    x_rows, d_rows = pl.pallas_call(
        pack_kernel,
        grid_spec=grid_spec,
        out_shape=[jax.ShapeDtypeStruct((cap, width), jnp.bfloat16)] * 2,
        compiler_params=pltpu.CompilerParams(dimension_semantics=("arbitrary",), vmem_limit_bytes=56 * 2**20),
        cost_estimate=pl.CostEstimate(flops=5 * CHUNK * cap * width, bytes_accessed=n_tok * width * 5, transcendentals=0),
        name="pack_rows",
    )(
        block_of.astype(jnp.int32),
        chunk_of.astype(jnp.int32),
        n_steps.astype(jnp.int32)[None],
        jnp.stack([my_exp, jnp.int32(n_exp)]),
        tokens,
        pos.astype(jnp.int32)[:, None, :],
        jnp.pad(w_router, ((0, 0), (0, 128 - n_exp))).astype(jnp.bfloat16),
    )
    return x_rows, d_rows, n_used.astype(jnp.int32)


def ffn_grads(hg, hu, da):
    hg, hu, da = (v.astype(jnp.bfloat16).astype(jnp.float32) for v in (hg, hu, da))
    sig = jax.nn.sigmoid(hg)
    silu = hg * sig
    act = (silu * hu).astype(jnp.bfloat16)
    dhu = (da * silu).astype(jnp.bfloat16)
    dhg = (da * hu * sig * (1.0 + hg * (1.0 - sig))).astype(jnp.bfloat16)
    return act, dhg, dhu


def own_kernel(r_ref, wg_ref, wu_ref, wd_ref, out_ref, wt_ref, acc_o, acc_x):
    j = pl.program_id(0)
    width = wd_ref.shape[1]
    x, d = r_ref[:, :width], r_ref[:, width:]

    @pl.when(j == 0)
    def _():
        acc_o[...] = jnp.zeros_like(acc_o)
        acc_x[...] = jnp.zeros_like(acc_x)

    wt_ref[0] = wg_ref[...].T
    wt_ref[1] = wu_ref[...].T
    hg = jnp.dot(x, wg_ref[...], preferred_element_type=jnp.float32)
    hu = jnp.dot(x, wu_ref[...], preferred_element_type=jnp.float32)
    da = lax.dot_general(wd_ref[...], d, NT, preferred_element_type=jnp.float32).astype(jnp.bfloat16).T
    act, dhg, dhu = ffn_grads(hg, hu, da)
    strip = width // 3 if width % 384 == 0 else width

    def add(i, carry):
        part = pl.ds(pl.multiple_of(i * strip, 128), strip)
        acc_o[:, part] += jnp.dot(act, wd_ref[:, part], preferred_element_type=jnp.float32)
        acc_x[part] += lax.dot_general(wg_ref[part], dhg, NT, preferred_element_type=jnp.float32) + lax.dot_general(wu_ref[part], dhu, NT, preferred_element_type=jnp.float32)
        return carry

    lax.fori_loop(0, width // strip, add, 0)

    @pl.when(j == pl.num_programs(0) - 1)
    def _():
        out_ref[:, :width] = acc_o[...].astype(jnp.bfloat16)
        out_ref[:, width:] = acc_x[...].astype(jnp.bfloat16).T


def own_rows(recv, w_gate, w_up, w_down):
    rows, two_d = recv.shape
    width, ff = w_gate.shape
    f = OWN_TILE
    whole = pl.BlockSpec((rows, two_d), lambda j: (0, 0))
    col_spec = pl.BlockSpec((width, f), lambda j: (0, j))
    return pl.pallas_call(
        own_kernel,
        grid=(ff // f,),
        in_specs=[whole, col_spec, col_spec, pl.BlockSpec((f, width), lambda j: (j, 0))],
        out_specs=[whole, pl.BlockSpec((2, f, width), lambda j: (0, j, 0))],
        out_shape=[jax.ShapeDtypeStruct((rows, two_d), jnp.bfloat16), jax.ShapeDtypeStruct((2, ff, width), jnp.bfloat16)],
        scratch_shapes=[pltpu.VMEM((rows, width), jnp.float32), pltpu.VMEM((width, rows), jnp.float32)],
        compiler_params=pltpu.CompilerParams(dimension_semantics=("arbitrary",), vmem_limit_bytes=62 * 2**20),
        cost_estimate=pl.CostEstimate(flops=12 * rows * width * ff, bytes_accessed=6 * width * ff, transcendentals=0),
        name="own_rows",
    )(recv, w_gate, w_up, w_down)


def tile_kernel(transpose, n_used, tile_of, block_of, x_ref, d_ref, wt_ref, wd_ref, *rest):
    outs, (acc_gu, acc_d, dgus, acts) = rest[:-4], rest[-4:]
    f = wd_ref.shape[0]
    step = pl.program_id(0)
    block = block_of[step]
    active = step < n_used[1]
    left = n_used[0] - GROUP * block

    def products(i, carry):
        at = pl.ds(pl.multiple_of(i * ROWS, ROWS), ROWS)
        wt = wt_ref[...].reshape(2 * f, wd_ref.shape[1])
        h = lax.dot_general(wt, x_ref[at], NT, preferred_element_type=jnp.float32)
        da = lax.dot_general(wd_ref[...], d_ref[at], NT, preferred_element_type=jnp.float32)
        acts[:, at], dgus[:f, at], dgus[f:, at] = ffn_grads(h[:f], h[f:], da)
        return carry

    @pl.when(active)
    def _():
        lax.fori_loop(0, jnp.minimum(left, GROUP), products, 0)

    def sums(rows):
        width = wd_ref.shape[1]
        strip = width // 3 if transpose and width % 384 == 0 else width

        def add(i, carry):
            cols = pl.ds(pl.multiple_of(i * strip, 128), strip)
            acc_gu[:, cols] = jnp.where(block == 0, 0.0, acc_gu[:, cols]) + jnp.dot(dgus[:, :rows], x_ref[:rows, cols], preferred_element_type=jnp.float32)
            acc_d[:, cols] = jnp.where(block == 0, 0.0, acc_d[:, cols]) + jnp.dot(acts[:, :rows], d_ref[:rows, cols], preferred_element_type=jnp.float32)
            return carry

        lax.fori_loop(0, width // strip, add, 0)

    for parts in range(1, GROUP + 1):
        fits = left >= parts if parts == GROUP else left == parts
        pl.when(active & fits)(functools.partial(sums, parts * ROWS))

    @pl.when(active & (left <= GROUP))
    def _():
        if transpose:
            outs[0][...] = acc_gu[:f].astype(jnp.bfloat16).T
            outs[1][...] = acc_gu[f:].astype(jnp.bfloat16).T
            outs[2][...] = acc_d[...].astype(jnp.bfloat16)
        else:
            outs[0][:2 * f] = acc_gu[...].astype(jnp.bfloat16)
            outs[0][2 * f:] = acc_d[...].astype(jnp.bfloat16)


def tile_grads(x_rows, d_rows, n_used, wt, wd, f, n_tile, ff):
    cap, width = x_rows.shape
    n_block = cap // (GROUP * ROWS)
    n_group = (n_used + GROUP - 1) // GROUP
    steps = jnp.arange(n_tile * n_block, dtype=jnp.int32)
    tile_of = jnp.minimum(steps // n_group, n_tile - 1)
    block_of = jnp.where(steps < n_tile * n_group, steps % n_group, n_group - 1)
    used = jnp.stack([n_used, n_tile * n_group])
    row_spec = pl.BlockSpec((GROUP * ROWS, width), lambda s, n, t, b: (b[s], 0))
    col_spec = pl.BlockSpec((width, f), lambda s, n, t, b: (0, t[s]))
    down_spec = pl.BlockSpec((f, width), lambda s, n, t, b: (t[s], 0))
    if ff:
        out_specs = [col_spec, col_spec, down_spec]
        out_shape = [jax.ShapeDtypeStruct((width, ff), jnp.bfloat16)] * 2 + [jax.ShapeDtypeStruct((ff, width), jnp.bfloat16)]
    else:
        out_specs = [pl.BlockSpec((3 * f, width), lambda s, n, t, b: (0, 0))]
        out_shape = [jax.ShapeDtypeStruct((3 * f, width), jnp.bfloat16)]
    return pl.pallas_call(
        functools.partial(tile_kernel, bool(ff)),
        grid_spec=pltpu.PrefetchScalarGridSpec(
            num_scalar_prefetch=3,
            grid=(n_tile * n_block,),
            in_specs=[row_spec, row_spec, pl.BlockSpec((2, f, width), lambda s, n, t, b: (0, t[s], 0)), down_spec],
            out_specs=out_specs,
            scratch_shapes=[
                pltpu.VMEM((2 * f, width), jnp.float32),
                pltpu.VMEM((f, width), jnp.float32),
                pltpu.VMEM((2 * f, GROUP * ROWS), jnp.bfloat16),
                pltpu.VMEM((f, GROUP * ROWS), jnp.bfloat16),
            ],
        ),
        out_shape=out_shape,
        compiler_params=pltpu.CompilerParams(dimension_semantics=("arbitrary",), vmem_limit_bytes=63 * 2**20),
        cost_estimate=pl.CostEstimate(flops=12 * (cap // 2) * width * f * n_tile, bytes_accessed=n_tile * cap * width * 2, transcendentals=0),
        name="tile_grads" if ff else "slice_grads",
    )(used, tile_of, block_of, x_rows, d_rows, wt, wd)


def place_kernel(part_ref, gg_in, gu_in, gd_in, gg_ref, gu_ref, gd_ref):
    f = SLICE
    gg_ref[...] = jnp.concatenate([part_ref[0, :f], part_ref[1, :f]], axis=0).T
    gu_ref[...] = jnp.concatenate([part_ref[0, f:2 * f], part_ref[1, f:2 * f]], axis=0).T
    gd_ref[:f] = part_ref[0, 2 * f:]
    gd_ref[f:] = part_ref[1, 2 * f:]


def place_slices(parts, g_gate, g_up, g_down, n_tile):
    n_part, _, width = parts.shape
    col_spec = pl.BlockSpec((width, 2 * SLICE), lambda i: (0, n_tile + i))
    down_spec = pl.BlockSpec((2 * SLICE, width), lambda i: (n_tile + i, 0))
    any_spec = pl.BlockSpec(memory_space=pl.ANY)
    return pl.pallas_call(
        place_kernel,
        grid=(n_part // 2,),
        in_specs=[pl.BlockSpec((2, 3 * SLICE, width), lambda i: (i, 0, 0)), any_spec, any_spec, any_spec],
        out_specs=[col_spec, col_spec, down_spec],
        out_shape=[jax.ShapeDtypeStruct(g.shape, g.dtype) for g in (g_gate, g_up, g_down)],
        input_output_aliases={1: 0, 2: 1, 3: 2},
        compiler_params=pltpu.CompilerParams(dimension_semantics=("arbitrary",), vmem_limit_bytes=50 * 2**20),
        cost_estimate=pl.CostEstimate(flops=10**6, bytes_accessed=4 * parts.size, transcendentals=0),
        name="place_slices",
    )(parts, g_gate, g_up, g_down)


def solution(mesh):
    n_dp, n_ep = mesh.shape["dp"], mesh.shape["ep"]
    n_dev = n_dp * n_ep
    all_axes = ("dp", "ep")

    def local_step(hidden, grad_out, expert_ids, norm_gain, w_router, w_gate, w_up, w_down):
        n_tok, width = hidden.shape
        n_exp = w_router.shape[1]
        capacity = 4 * n_tok // n_exp
        total_tok = n_tok * n_dev
        w_gate, w_up, w_down = w_gate[0], w_up[0], w_down[0]
        ff = w_gate.shape[1]
        n_tile = (ff - SLICE * n_dp) // TILE
        my_exp = lax.axis_index("ep")
        dest_rows, slot_owner = route_tables(expert_ids, n_exp, capacity)
        choice_hot = (expert_ids[:, :, None] == jnp.arange(n_exp, dtype=jnp.int32)).astype(jnp.float32)

        x_f32 = hidden.astype(jnp.float32)
        inv_rms = lax.rsqrt(jnp.mean(x_f32 * x_f32, axis=-1, keepdims=True) + EPS)
        x_hat = x_f32 * inv_rms
        x_norm = (x_hat * norm_gain).astype(jnp.bfloat16)
        xn_f32 = x_norm.astype(jnp.float32)

        tokens = lax.all_gather(jnp.concatenate([x_norm, grad_out], axis=1), all_axes, axis=0, tiled=True)

        router_probs = jax.nn.softmax(jnp.dot(xn_f32, w_router, preferred_element_type=jnp.float32), axis=-1)
        gate_vals = jnp.sum(router_probs[:, None, :] * choice_hot, axis=-1)

        dy_f32 = grad_out.astype(jnp.float32)
        d_picked = (dy_f32[:, None, :] * gate_vals[:, :, None]).astype(jnp.bfloat16).reshape(n_tok * 2, width)
        send_x = jnp.take(x_norm, slot_owner // 2, axis=0, mode="fill", fill_value=0)
        send_d = jnp.take(d_picked, slot_owner, axis=0, mode="fill", fill_value=0)
        send = jnp.concatenate([send_x, send_d], axis=1).reshape(n_exp, capacity, 2 * width)
        recv = lax.all_to_all(send, "ep", 0, 0, tiled=True).reshape(n_exp * capacity, 2 * width)
        home, wt = own_rows(recv, w_gate, w_up, w_down)

        pad = jnp.zeros((n_tok, 16 - n_exp - 2), jnp.float32)
        routes = jnp.concatenate([router_probs, expert_ids.astype(jnp.float32), pad], axis=1)
        routes, home = lax.optimization_barrier((routes, home))
        routes = lax.all_gather(routes, all_axes, axis=0, tiled=True)
        all_probs, all_ids = routes[:, :n_exp], routes[:, n_exp:n_exp + 2].astype(jnp.int32)
        exp_range = jnp.arange(n_exp, dtype=jnp.int32)
        loads = jnp.sum((all_ids[:, 0:1] == exp_range).astype(jnp.float32) + (all_ids[:, 1:2] == exp_range).astype(jnp.float32), axis=0)
        load_frac = loads / (2 * total_tok)
        aux_loss = AUX_COEF * n_exp * jnp.sum(load_frac * jnp.sum(all_probs, axis=0) / total_tok)

        home = home.reshape(n_exp, capacity, 2 * width)
        back = lax.all_to_all(home, "ep", 0, 0, tiled=True).reshape(n_exp * capacity, 2 * width)
        taken = jnp.take(back, dest_rows, axis=0).reshape(n_tok, 2, 2 * width)
        picked, d_xn_exp = taken[:, :, :width], taken[:, :, width:]
        out_hidden = (x_f32 + jnp.sum(gate_vals[:, :, None] * picked, axis=1)).astype(jnp.bfloat16)

        d_gates = jnp.sum(dy_f32[:, None, :] * picked, axis=-1)
        d_probs = jnp.sum(d_gates[:, :, None] * choice_hot, axis=1) + (AUX_COEF * n_exp / total_tok) * load_frac
        d_logits = router_probs * (d_probs - jnp.sum(router_probs * d_probs, axis=-1, keepdims=True))
        d_xnorm = jnp.einsum("te,de->td", d_logits, w_router) + d_xn_exp[:, 0].astype(jnp.float32) + d_xn_exp[:, 1].astype(jnp.float32)
        d_xnorm = d_xnorm.astype(jnp.bfloat16).astype(jnp.float32)
        scaled = d_xnorm * norm_gain
        grad_hidden = (inv_rms * (scaled - x_hat * jnp.mean(scaled * x_hat, axis=-1, keepdims=True)) + dy_f32).astype(jnp.bfloat16)
        small = [jnp.sum(d_xnorm * x_hat, axis=0), jnp.einsum("te,td->ed", d_logits, xn_f32).reshape(-1)]
        small = lax.all_gather(jnp.concatenate(small).reshape(-1, 128), all_axes, axis=0, tiled=True)
        small = jnp.sum(small.reshape(n_dev, -1, 128), axis=0).reshape(1 + n_exp, width)

        at = n_tile * TILE + SLICE * lax.axis_index("dp")
        wt_mine = lax.dynamic_slice(wt, (0, at, 0), (2, SLICE, width))
        wd_mine = lax.dynamic_slice(w_down, (at, 0), (SLICE, width))
        names = all_ids == my_exp
        x_rows, do_rows, n_used = pack_rows(tokens, width, names[:, 0] | names[:, 1], w_router, my_exp, n_dev * capacity)
        (mine,) = tile_grads(x_rows, do_rows, n_used, wt_mine, wd_mine, SLICE, 1, 0)
        parts = lax.all_gather(mine, "dp", axis=0, tiled=False)
        grads = tile_grads(x_rows, do_rows, n_used, wt, w_down, TILE, n_tile, ff)
        g_gate, g_up, g_down = place_slices(parts, *grads, n_tile)
        return (out_hidden, aux_loss, grad_hidden, small[0], small[1:].T, g_gate[None], g_up[None], g_down[None])

    tok_spec = P(all_axes, None)
    w_spec = P("ep", None, None)
    return jax.shard_map(local_step, mesh=mesh, in_specs=(tok_spec, tok_spec, tok_spec, P(), P(), w_spec, w_spec, w_spec), out_specs=(tok_spec, P(), tok_spec, P(), P(), w_spec, w_spec, w_spec), check_vma=False)
```

```python
import functools
import jax
import jax.numpy as jnp
from jax import lax
from jax.experimental import pallas as pl
from jax.experimental.pallas import tpu as pltpu
from jax.sharding import PartitionSpec as P

EPS = 1e-6
AUX_COEF = 0.001
ROWS = 256
GROUP = 2
CHUNK = 512
STRIP = 512
BUFFERS = 3
OWN_TILE = 640
TILE = 384
SLICE = 192
NT = (((1,), (1,)), ((), ()))


def route_tables(expert_ids, n_exp, capacity):
    flat_ids = expert_ids.reshape(-1)
    n_choice = flat_ids.shape[0]
    one_hot = (flat_ids[:, None] == jnp.arange(n_exp, dtype=jnp.int32)[None, :]).astype(jnp.int32)
    running = jnp.cumsum(one_hot, axis=0) - 1
    dest_rows = flat_ids * capacity + jnp.sum(running * one_hot, axis=1)
    slot_owner = jnp.full((n_exp * capacity,), n_choice, jnp.int32).at[dest_rows].set(jnp.arange(n_choice, dtype=jnp.int32))
    return dest_rows, slot_owner


def pack_kernel(block_of, chunk_of, n_steps, my_exp, tok_hbm, pos_ref, wr_ref, x_ref, d_ref, acc, ring, sems):
    step = pl.program_id(0)
    rows, width = x_ref.shape
    block = block_of[step]
    active = step < n_steps[0]
    chunk = chunk_of[step]
    last_chunk = chunk_of[n_steps[0] - 1]

    def load(c):
        slot = lax.rem(c, BUFFERS)
        return pltpu.make_async_copy(tok_hbm.at[pl.ds(pl.multiple_of(c * CHUNK, CHUNK), CHUNK), pl.ds(0, ring.shape[2])], ring.at[slot], sems.at[slot])

    @pl.when(step == 0)
    def _():
        for c in range(BUFFERS - 1):
            pl.when(c <= last_chunk)(load(c).start)

    @pl.when(active & ((step == 0) | (chunk != chunk_of[jnp.maximum(step - 1, 0)])))
    def _():
        load(chunk).wait()
        pl.when(chunk + BUFFERS - 1 <= last_chunk)(load(chunk + BUFFERS - 1).start)

    tok_ref = ring.at[lax.rem(chunk, BUFFERS)]
    new = (step == 0) | (block != block_of[jnp.maximum(step - 1, 0)])

    @pl.when(active)
    def _():
        row_id = block * rows + lax.broadcasted_iota(jnp.int32, (rows, tok_ref.shape[0]), 0)
        hit = (pos_ref[0] == row_id).astype(jnp.float32).astype(jnp.bfloat16)
        for at in range(0, 2 * width, STRIP):
            cols = slice(at, at + STRIP)
            acc[:, cols] = jnp.where(new, 0.0, acc[:, cols]) + jnp.dot(hit, tok_ref[:, cols], preferred_element_type=jnp.float32)

    @pl.when((step == n_steps[0] - 1) | (active & (block != block_of[step + 1])))
    def _():
        x = acc[:, :width].astype(jnp.bfloat16)
        logits = jnp.dot(x, wr_ref[...], preferred_element_type=jnp.float32)
        lane = lax.broadcasted_iota(jnp.int32, logits.shape, 1)
        logits = jnp.where(lane < my_exp[1], logits, -jnp.inf)
        p = jnp.exp(logits - jnp.max(logits, axis=1, keepdims=True))
        gate = jnp.sum(jnp.where(lane == my_exp[0], p, 0.0), axis=1, keepdims=True) / jnp.sum(p, axis=1, keepdims=True)
        x_ref[...] = x
        d_ref[...] = (acc[:, width:] * gate).astype(jnp.bfloat16)


def pack_rows(tokens, width, mask, w_router, my_exp, cap):
    n_tok = tokens.shape[0]
    n_exp = w_router.shape[1]
    n_chunk = n_tok // CHUNK
    n_block = cap // ROWS
    m = mask.astype(jnp.bfloat16).reshape(n_chunk, CHUNK)
    idx = jnp.arange(CHUNK)
    inside = jnp.dot(m, (idx[:, None] < idx[None, :]).astype(jnp.bfloat16), preferred_element_type=jnp.float32).astype(jnp.int32)
    per_chunk = jnp.sum(mask.astype(jnp.int32).reshape(n_chunk, CHUNK), axis=1)
    cidx = jnp.arange(n_chunk)
    ends = jnp.sum(jnp.where(cidx[None, :] <= cidx[:, None], per_chunk[None, :], 0), axis=1)
    pos = jnp.where(mask.reshape(n_chunk, CHUNK), inside + (ends - per_chunk)[:, None], -1)
    count = jnp.sum(per_chunk)
    n_used = jnp.maximum((count + ROWS - 1) // ROWS, 1)
    bidx = jnp.arange(n_block)
    last_row = jnp.minimum((bidx + 1) * ROWS, count) - 1
    last_chunk = jnp.sum((ends[None, :] <= last_row[:, None]).astype(jnp.int32), axis=1)
    n_steps = jnp.sum(jnp.where(bidx == n_used - 1, last_chunk + bidx, 0)) + 1
    steps = jnp.arange(n_chunk + n_block + 1)
    block_of = jnp.minimum(jnp.sum(((last_chunk + bidx)[None, :] < steps[:, None]).astype(jnp.int32), axis=1), n_used - 1)
    chunk_of = jnp.clip(steps - block_of, 0, n_chunk - 1)
    chunk_of = jnp.where(steps < n_steps, chunk_of, n_chunk - 1)
    grid_spec = pltpu.PrefetchScalarGridSpec(
        num_scalar_prefetch=4,
        grid=(n_chunk + n_block,),
        in_specs=[
            pl.BlockSpec(memory_space=pl.ANY),
            pl.BlockSpec((1, 1, CHUNK), lambda s, b, c, n, e: (c[s], 0, 0)),
            pl.BlockSpec((width, 128), lambda s, b, c, n, e: (0, 0)),
        ],
        out_specs=[pl.BlockSpec((ROWS, width), lambda s, b, c, n, e: (b[s], 0))] * 2,
        scratch_shapes=[
            pltpu.VMEM((ROWS, 2 * width), jnp.float32),
            pltpu.VMEM((BUFFERS, CHUNK, 2 * width), jnp.bfloat16),
            pltpu.SemaphoreType.DMA((BUFFERS,)),
        ],
    )
    x_rows, d_rows = pl.pallas_call(
        pack_kernel,
        grid_spec=grid_spec,
        out_shape=[jax.ShapeDtypeStruct((cap, width), jnp.bfloat16)] * 2,
        compiler_params=pltpu.CompilerParams(dimension_semantics=("arbitrary",), vmem_limit_bytes=56 * 2**20),
        cost_estimate=pl.CostEstimate(flops=5 * CHUNK * cap * width, bytes_accessed=n_tok * width * 5, transcendentals=0),
        name="pack_rows",
    )(
        block_of.astype(jnp.int32),
        chunk_of.astype(jnp.int32),
        n_steps.astype(jnp.int32)[None],
        jnp.stack([my_exp, jnp.int32(n_exp)]),
        tokens,
        pos.astype(jnp.int32)[:, None, :],
        jnp.pad(w_router, ((0, 0), (0, 128 - n_exp))).astype(jnp.bfloat16),
    )
    return x_rows, d_rows, n_used.astype(jnp.int32)


def ffn_grads(hg, hu, da):
    hg, hu, da = (v.astype(jnp.bfloat16).astype(jnp.float32) for v in (hg, hu, da))
    sig = jax.nn.sigmoid(hg)
    silu = hg * sig
    act = (silu * hu).astype(jnp.bfloat16)
    dhu = (da * silu).astype(jnp.bfloat16)
    dhg = (da * hu * sig * (1.0 + hg * (1.0 - sig))).astype(jnp.bfloat16)
    return act, dhg, dhu


def own_kernel(r_ref, wg_ref, wu_ref, wd_ref, out_ref, wt_ref, acc_o, acc_x):
    j = pl.program_id(0)
    width = wd_ref.shape[1]
    x, d = r_ref[:, :width], r_ref[:, width:]

    @pl.when(j == 0)
    def _():
        acc_o[...] = jnp.zeros_like(acc_o)
        acc_x[...] = jnp.zeros_like(acc_x)

    wt_ref[0] = wg_ref[...].T
    wt_ref[1] = wu_ref[...].T
    hg = jnp.dot(x, wg_ref[...], preferred_element_type=jnp.float32)
    hu = jnp.dot(x, wu_ref[...], preferred_element_type=jnp.float32)
    da = lax.dot_general(wd_ref[...], d, NT, preferred_element_type=jnp.float32).astype(jnp.bfloat16).T
    act, dhg, dhu = ffn_grads(hg, hu, da)
    strip = width // 3 if width % 384 == 0 else width

    def add(i, carry):
        part = pl.ds(pl.multiple_of(i * strip, 128), strip)
        acc_o[:, part] += jnp.dot(act, wd_ref[:, part], preferred_element_type=jnp.float32)
        acc_x[part] += lax.dot_general(wg_ref[part], dhg, NT, preferred_element_type=jnp.float32) + lax.dot_general(wu_ref[part], dhu, NT, preferred_element_type=jnp.float32)
        return carry

    lax.fori_loop(0, width // strip, add, 0)

    @pl.when(j == pl.num_programs(0) - 1)
    def _():
        out_ref[:, :width] = acc_o[...].astype(jnp.bfloat16)
        out_ref[:, width:] = acc_x[...].astype(jnp.bfloat16).T


def own_rows(recv, w_gate, w_up, w_down):
    rows, two_d = recv.shape
    width, ff = w_gate.shape
    f = OWN_TILE
    whole = pl.BlockSpec((rows, two_d), lambda j: (0, 0))
    col_spec = pl.BlockSpec((width, f), lambda j: (0, j))
    return pl.pallas_call(
        own_kernel,
        grid=(ff // f,),
        in_specs=[whole, col_spec, col_spec, pl.BlockSpec((f, width), lambda j: (j, 0))],
        out_specs=[whole, pl.BlockSpec((2, f, width), lambda j: (0, j, 0))],
        out_shape=[jax.ShapeDtypeStruct((rows, two_d), jnp.bfloat16), jax.ShapeDtypeStruct((2, ff, width), jnp.bfloat16)],
        scratch_shapes=[pltpu.VMEM((rows, width), jnp.float32), pltpu.VMEM((width, rows), jnp.float32)],
        compiler_params=pltpu.CompilerParams(dimension_semantics=("arbitrary",), vmem_limit_bytes=62 * 2**20),
        cost_estimate=pl.CostEstimate(flops=12 * rows * width * ff, bytes_accessed=6 * width * ff, transcendentals=0),
        name="own_rows",
    )(recv, w_gate, w_up, w_down)


def tile_kernel(transpose, n_used, tile_of, block_of, x_ref, d_ref, wt_ref, wd_ref, *rest):
    outs, (acc_gu, acc_d, dgus, acts) = rest[:-4], rest[-4:]
    f = wd_ref.shape[0]
    step = pl.program_id(0)
    block = block_of[step]
    active = step < n_used[1]
    left = n_used[0] - GROUP * block

    def products(i, carry):
        at = pl.ds(pl.multiple_of(i * ROWS, ROWS), ROWS)
        wt = wt_ref[...].reshape(2 * f, wd_ref.shape[1])
        h = lax.dot_general(wt, x_ref[at], NT, preferred_element_type=jnp.float32)
        da = lax.dot_general(wd_ref[...], d_ref[at], NT, preferred_element_type=jnp.float32)
        acts[:, at], dgus[:f, at], dgus[f:, at] = ffn_grads(h[:f], h[f:], da)
        return carry

    @pl.when(active)
    def _():
        lax.fori_loop(0, jnp.minimum(left, GROUP), products, 0)

    def sums(rows):
        width = wd_ref.shape[1]
        strip = width // 3 if transpose and width % 384 == 0 else width

        def add(i, carry):
            cols = pl.ds(pl.multiple_of(i * strip, 128), strip)
            acc_gu[:, cols] = jnp.where(block == 0, 0.0, acc_gu[:, cols]) + jnp.dot(dgus[:, :rows], x_ref[:rows, cols], preferred_element_type=jnp.float32)
            acc_d[:, cols] = jnp.where(block == 0, 0.0, acc_d[:, cols]) + jnp.dot(acts[:, :rows], d_ref[:rows, cols], preferred_element_type=jnp.float32)
            return carry

        lax.fori_loop(0, width // strip, add, 0)

    for parts in range(1, GROUP + 1):
        fits = left >= parts if parts == GROUP else left == parts
        pl.when(active & fits)(functools.partial(sums, parts * ROWS))

    @pl.when(active & (left <= GROUP))
    def _():
        if transpose:
            outs[0][...] = acc_gu[:f].astype(jnp.bfloat16).T
            outs[1][...] = acc_gu[f:].astype(jnp.bfloat16).T
            outs[2][...] = acc_d[...].astype(jnp.bfloat16)
        else:
            outs[0][:2 * f] = acc_gu[...].astype(jnp.bfloat16)
            outs[0][2 * f:] = acc_d[...].astype(jnp.bfloat16)


def tile_grads(x_rows, d_rows, n_used, wt, wd, f, n_tile, ff):
    cap, width = x_rows.shape
    n_block = cap // (GROUP * ROWS)
    n_group = (n_used + GROUP - 1) // GROUP
    steps = jnp.arange(n_tile * n_block, dtype=jnp.int32)
    tile_of = jnp.minimum(steps // n_group, n_tile - 1)
    block_of = jnp.where(steps < n_tile * n_group, steps % n_group, n_group - 1)
    used = jnp.stack([n_used, n_tile * n_group])
    row_spec = pl.BlockSpec((GROUP * ROWS, width), lambda s, n, t, b: (b[s], 0))
    col_spec = pl.BlockSpec((width, f), lambda s, n, t, b: (0, t[s]))
    down_spec = pl.BlockSpec((f, width), lambda s, n, t, b: (t[s], 0))
    if ff:
        out_specs = [col_spec, col_spec, down_spec]
        out_shape = [jax.ShapeDtypeStruct((width, ff), jnp.bfloat16)] * 2 + [jax.ShapeDtypeStruct((ff, width), jnp.bfloat16)]
    else:
        out_specs = [pl.BlockSpec((3 * f, width), lambda s, n, t, b: (0, 0))]
        out_shape = [jax.ShapeDtypeStruct((3 * f, width), jnp.bfloat16)]
    return pl.pallas_call(
        functools.partial(tile_kernel, bool(ff)),
        grid_spec=pltpu.PrefetchScalarGridSpec(
            num_scalar_prefetch=3,
            grid=(n_tile * n_block,),
            in_specs=[row_spec, row_spec, pl.BlockSpec((2, f, width), lambda s, n, t, b: (0, t[s], 0)), down_spec],
            out_specs=out_specs,
            scratch_shapes=[
                pltpu.VMEM((2 * f, width), jnp.float32),
                pltpu.VMEM((f, width), jnp.float32),
                pltpu.VMEM((2 * f, GROUP * ROWS), jnp.bfloat16),
                pltpu.VMEM((f, GROUP * ROWS), jnp.bfloat16),
            ],
        ),
        out_shape=out_shape,
        compiler_params=pltpu.CompilerParams(dimension_semantics=("arbitrary",), vmem_limit_bytes=63 * 2**20),
        cost_estimate=pl.CostEstimate(flops=12 * (cap // 2) * width * f * n_tile, bytes_accessed=n_tile * cap * width * 2, transcendentals=0),
        name="tile_grads" if ff else "slice_grads",
    )(used, tile_of, block_of, x_rows, d_rows, wt, wd)


def place_kernel(part_ref, gg_in, gu_in, gd_in, gg_ref, gu_ref, gd_ref):
    f = SLICE
    gg_ref[...] = jnp.concatenate([part_ref[0, :f], part_ref[1, :f]], axis=0).T
    gu_ref[...] = jnp.concatenate([part_ref[0, f:2 * f], part_ref[1, f:2 * f]], axis=0).T
    gd_ref[:f] = part_ref[0, 2 * f:]
    gd_ref[f:] = part_ref[1, 2 * f:]


def place_slices(parts, g_gate, g_up, g_down, n_tile):
    n_part, _, width = parts.shape
    col_spec = pl.BlockSpec((width, 2 * SLICE), lambda i: (0, n_tile + i))
    down_spec = pl.BlockSpec((2 * SLICE, width), lambda i: (n_tile + i, 0))
    any_spec = pl.BlockSpec(memory_space=pl.ANY)
    return pl.pallas_call(
        place_kernel,
        grid=(n_part // 2,),
        in_specs=[pl.BlockSpec((2, 3 * SLICE, width), lambda i: (i, 0, 0)), any_spec, any_spec, any_spec],
        out_specs=[col_spec, col_spec, down_spec],
        out_shape=[jax.ShapeDtypeStruct(g.shape, g.dtype) for g in (g_gate, g_up, g_down)],
        input_output_aliases={1: 0, 2: 1, 3: 2},
        compiler_params=pltpu.CompilerParams(dimension_semantics=("arbitrary",), vmem_limit_bytes=50 * 2**20),
        cost_estimate=pl.CostEstimate(flops=10**6, bytes_accessed=4 * parts.size, transcendentals=0),
        name="place_slices",
    )(parts, g_gate, g_up, g_down)


def solution(mesh):
    n_dp, n_ep = mesh.shape["dp"], mesh.shape["ep"]
    n_dev = n_dp * n_ep
    all_axes = ("dp", "ep")

    def local_step(hidden, grad_out, expert_ids, norm_gain, w_router, w_gate, w_up, w_down):
        n_tok, width = hidden.shape
        n_exp = w_router.shape[1]
        capacity = 4 * n_tok // n_exp
        total_tok = n_tok * n_dev
        w_gate, w_up, w_down = w_gate[0], w_up[0], w_down[0]
        ff = w_gate.shape[1]
        n_tile = (ff - SLICE * n_dp) // TILE
        my_exp = lax.axis_index("ep")
        dest_rows, slot_owner = route_tables(expert_ids, n_exp, capacity)
        choice_hot = (expert_ids[:, :, None] == jnp.arange(n_exp, dtype=jnp.int32)).astype(jnp.float32)

        x_f32 = hidden.astype(jnp.float32)
        inv_rms = lax.rsqrt(jnp.mean(x_f32 * x_f32, axis=-1, keepdims=True) + EPS)
        x_hat = x_f32 * inv_rms
        x_norm = (x_hat * norm_gain).astype(jnp.bfloat16)
        xn_f32 = x_norm.astype(jnp.float32)

        tokens = lax.all_gather(jnp.concatenate([x_norm, grad_out, jnp.pad(expert_ids.astype(jnp.bfloat16), ((0, 0), (0, 126)))], axis=1), all_axes, axis=0, tiled=True)

        router_probs = jax.nn.softmax(jnp.dot(xn_f32, w_router, preferred_element_type=jnp.float32), axis=-1)
        gate_vals = jnp.sum(router_probs[:, None, :] * choice_hot, axis=-1)

        dy_f32 = grad_out.astype(jnp.float32)
        d_picked = (dy_f32[:, None, :] * gate_vals[:, :, None]).astype(jnp.bfloat16).reshape(n_tok * 2, width)
        send_x = jnp.take(x_norm, slot_owner // 2, axis=0, mode="fill", fill_value=0)
        send_d = jnp.take(d_picked, slot_owner, axis=0, mode="fill", fill_value=0)
        send = jnp.concatenate([send_x, send_d], axis=1).reshape(n_exp, capacity, 2 * width)
        recv = lax.all_to_all(send, "ep", 0, 0, tiled=True).reshape(n_exp * capacity, 2 * width)
        home, wt = own_rows(recv, w_gate, w_up, w_down)

        exp_range = jnp.arange(n_exp, dtype=jnp.int32)
        home = home.reshape(n_exp, capacity, 2 * width)
        back = lax.all_to_all(home, "ep", 0, 0, tiled=True).reshape(n_exp * capacity, 2 * width)
        taken = jnp.take(back, dest_rows, axis=0).reshape(n_tok, 2, 2 * width)
        picked, d_xn_exp = taken[:, :, :width], taken[:, :, width:]
        out_hidden = (x_f32 + jnp.sum(gate_vals[:, :, None] * picked, axis=1)).astype(jnp.bfloat16)

        all_ids = tokens[:, 2 * width:2 * width + 2].astype(jnp.int32)
        loads = jnp.sum((all_ids[:, 0:1] == exp_range).astype(jnp.float32) + (all_ids[:, 1:2] == exp_range).astype(jnp.float32), axis=0)
        load_frac = loads / (2 * total_tok)
        d_gates = jnp.sum(dy_f32[:, None, :] * picked, axis=-1)
        d_probs = jnp.sum(d_gates[:, :, None] * choice_hot, axis=1) + (AUX_COEF * n_exp / total_tok) * load_frac
        d_logits = router_probs * (d_probs - jnp.sum(router_probs * d_probs, axis=-1, keepdims=True))
        d_xnorm = jnp.einsum("te,de->td", d_logits, w_router) + d_xn_exp[:, 0].astype(jnp.float32) + d_xn_exp[:, 1].astype(jnp.float32)
        d_xnorm = d_xnorm.astype(jnp.bfloat16).astype(jnp.float32)
        scaled = d_xnorm * norm_gain
        grad_hidden = (inv_rms * (scaled - x_hat * jnp.mean(scaled * x_hat, axis=-1, keepdims=True)) + dy_f32).astype(jnp.bfloat16)
        small = [jnp.sum(d_xnorm * x_hat, axis=0), jnp.einsum("te,td->ed", d_logits, xn_f32).reshape(-1), jnp.pad(jnp.sum(router_probs, axis=0), (0, 128 - n_exp))]
        small = lax.all_gather(jnp.concatenate(small).reshape(-1, 128), all_axes, axis=0, tiled=True)
        small = jnp.sum(small.reshape(n_dev, -1, 128), axis=0)
        aux_loss = AUX_COEF * n_exp * jnp.sum(load_frac * small[-1, :n_exp] / total_tok)
        small = small[:-1].reshape(1 + n_exp, width)

        at = n_tile * TILE + SLICE * lax.axis_index("dp")
        wt_mine = lax.dynamic_slice(wt, (0, at, 0), (2, SLICE, width))
        wd_mine = lax.dynamic_slice(w_down, (at, 0), (SLICE, width))
        names = all_ids == my_exp
        x_rows, do_rows, n_used = pack_rows(tokens, width, names[:, 0] | names[:, 1], w_router, my_exp, n_dev * capacity)
        (mine,) = tile_grads(x_rows, do_rows, n_used, wt_mine, wd_mine, SLICE, 1, 0)
        parts = lax.all_gather(mine, "dp", axis=0, tiled=False)
        grads = tile_grads(x_rows, do_rows, n_used, wt, w_down, TILE, n_tile, ff)
        g_gate, g_up, g_down = place_slices(parts, *grads, n_tile)
        return (out_hidden, aux_loss, grad_hidden, small[0], small[1:].T, g_gate[None], g_up[None], g_down[None])

    tok_spec = P(all_axes, None)
    w_spec = P("ep", None, None)
    return jax.shard_map(local_step, mesh=mesh, in_specs=(tok_spec, tok_spec, tok_spec, P(), P(), w_spec, w_spec, w_spec), out_specs=(tok_spec, P(), tok_spec, P(), P(), w_spec, w_spec, w_spec), check_vma=False)
```
